256 devices in a mesh: shift: 4 (over x), fsdp: 32 (over z, y_lo, core), tp: 2 (over y_hi).
Axes of the slice: x: 4, y: 4 (y_hi: 2, y_lo: 2; y = y_hi * 2 + y_lo), z: 8, core: 2. Of those that a mesh axis runs over, the one named last changes fastest.
Arguments:
- grad_stack: float32 [512, 128, 2048], P('shift', 'fsdp', 'tp'), parts along dimension 0, may hold values from -6 to 6
- moment_stack: float32 [512, 128, 2048], P('shift', 'fsdp', 'tp'), parts along dimension 0, may hold values from -6 to 6
- weight_stack: float32 [512, 128, 2048], P('shift', 'fsdp', 'tp'), parts along dimension 0, may hold values from -0.1875 to 0.1875
Outputs:
- new_weights: float32 [512, 128, 2048], P('shift', 'fsdp', 'tp'), parts along dimension 0
- new_momentum: float32 [512, 128, 2048], P('shift', 'fsdp', 'tp'), parts along dimension 0
The draws below stay inside these ranges and needn't reach their ends.
There are 4 independent parts, one for each index of `shift`. The reference program is written for one: setup_inputs(seed, part) draws one part's arguments, and reference() takes and returns one part's arrays. A program takes and returns all parts, laid end to end along the dimension named above; each array names one. Nothing has to cross between parts.
All inputs are finite; a program needn't handle non-finite values.
Results may differ from the reference program's by a relative error of at most 0.0003.
Values sent between devices are 32-bit elements.
No kernel may reach another device: no remote copies, remote signals or barrier semaphores. Data moves between devices by JAX's collectives and lax.ppermute only.
A program may use at most 64 MiB of HBM per device.

```python
import jax
import jax.numpy as jnp
from jax import lax

SIDE = 128
WIDE = 2048
MATS = 128
ITERS = 3


def block_scale(key, dims, cuts, smallest, largest):
    loudness, own = 1.0, jax.random.fold_in(key, 6)
    for position, parts in cuts:
        draws = jnp.exp(jax.random.uniform(jax.random.fold_in(own, position), (parts,), jnp.float32, smallest / len(cuts), largest / len(cuts)))
        loudness = loudness * jnp.repeat(draws, dims[position] // parts).reshape([-1 if axis == position else 1 for axis in range(len(dims))])
    return loudness


def gaussian(rng, shape, spread, reach, split=(), dtype=jnp.bfloat16):
    factor_of = block_scale(rng, shape, split, -0.22, 0.18) if split else 1.0
    array = jax.random.normal(rng, shape, jnp.float32) * spread * factor_of
    return jnp.minimum(jnp.maximum(array, -reach), reach).astype(dtype)


def setup_inputs(seed: int = 0, part: int = 0) -> dict:
    key_list = jax.random.split(jax.random.key(seed), 4)
    part_splits = jax.random.split(jax.random.fold_in(key_list[3], part), 4)
    grad_stack = gaussian(part_splits[0], (MATS, SIDE, WIDE), 1.0, 6.0, ((1, 32), (2, 2)), jnp.float32)
    moment_stack = gaussian(part_splits[1], (MATS, SIDE, WIDE), 1.0, 6.0, ((1, 32), (2, 2)), jnp.float32)
    weight_stack = gaussian(part_splits[2], (MATS, SIDE, WIDE), 0.03, 0.1875, ((1, 32), (2, 2)), jnp.float32)
    return dict(grad_stack=grad_stack, moment_stack=moment_stack, weight_stack=weight_stack)


hold_rate = 0.95
learn_rate = 0.9

def reference(grad_stack, moment_stack, weight_stack):
    new_momentum = hold_rate * moment_stack + grad_stack

    def orthogonal_one(stack):
        iterate = stack[None]
        iterate = iterate * lax.rsqrt(lax.optimization_barrier(jnp.sum(iterate * iterate, axis=(1, 2), keepdims=True)) + 1e-06)
        for step in range(ITERS):
            gram = jnp.einsum('mik,mjk->mij', iterate, iterate, precision=lax.Precision.HIGHEST)
            mixed = -4.775 * gram + 2.0315 * jnp.einsum('mij,mjk->mik', gram, gram, precision=lax.Precision.HIGHEST)
            iterate = 3.4445 * iterate + jnp.einsum('mij,mjk->mik', mixed, iterate, precision=lax.Precision.HIGHEST)
        return iterate[0]
    iterate = lax.map(orthogonal_one, new_momentum)
    new_weights = weight_stack - learn_rate * iterate
    return (new_weights, new_momentum)
```

```python
import functools

import jax
import jax.numpy as jnp
from jax import lax
from jax.experimental import pallas as pl
from jax.experimental.pallas import tpu as pltpu
from jax.sharding import PartitionSpec as P

ITERS = 3
CHUNKS = 1


hold_rate = 0.95
learn_rate = 0.9

dot = functools.partial(
    lax.dot_general, precision=lax.Precision.HIGHEST, preferred_element_type=jnp.float32
)
ROW_BY_ROW = (((1,), (1,)), ((), ()))
PLAIN = (((1,), (0,)), ((), ()))


def step_matrix(gram):
    side = gram.shape[0]
    row = lax.broadcasted_iota(jnp.int32, (side, side), 0)
    col = lax.broadcasted_iota(jnp.int32, (side, side), 1)
    diagonal = row == col
    total = jnp.sum(jnp.where(diagonal, gram, 0.0))
    inverse = lax.rsqrt(total + 1e-06)
    gram = (gram * inverse) * inverse
    product = None
    for step in range(ITERS):
        square = dot(gram, gram, PLAIN)
        factor = jnp.where(diagonal, 3.4445, 0.0) + (-4.775 * gram + 2.0315 * square)
        if step < ITERS - 1:
            gram = dot(dot(factor, gram, PLAIN), factor, PLAIN)
        product = factor if product is None else dot(factor, product, PLAIN)
    return product * (learn_rate * inverse)


def matrix_kernel(moved_ref, out_ref, whole_ref):
    rows, halves, few, wide = moved_ref.shape[1:]
    for row in range(rows):
        for half in range(halves):
            whole_ref[row * few : (row + 1) * few, half * wide : (half + 1) * wide] = moved_ref[0, row, half]
    whole = whole_ref[...]
    gram = dot(whole, whole, ROW_BY_ROW)
    whole_ref[...] = dot(step_matrix(gram), whole, PLAIN)
    for row in range(rows):
        for half in range(halves):
            out_ref[0, row, half] = whole_ref[row * few : (row + 1) * few, half * wide : (half + 1) * wide]


def update_matrices(moved):
    mats, rows, halves, few, wide = moved.shape
    side, width = rows * few, halves * wide
    flops = mats * (6 * 2) * (2 * side * side * width + 9 * side**3)
    block = pl.BlockSpec((1, rows, halves, few, wide), lambda m: (m, 0, 0, 0, 0))
    return pl.pallas_call(
        matrix_kernel,
        grid=(mats,),
        out_shape=jax.ShapeDtypeStruct(moved.shape, jnp.float32),
        in_specs=[block],
        out_specs=block,
        scratch_shapes=[pltpu.VMEM((side, width), jnp.float32)],
        cost_estimate=pl.CostEstimate(flops=flops, bytes_accessed=2 * 4 * moved.size, transcendentals=0),
    )(moved)


def body(grad_stack, moment_stack, weight_stack):
    mats, few, wide = grad_stack.shape
    rows, halves = lax.axis_size("fsdp"), lax.axis_size("tp")
    group = rows * halves
    own = mats // CHUNKS // group
    new_momentum = hold_rate * moment_stack + grad_stack
    pieces = []
    for chunk in jnp.split(new_momentum, CHUNKS):
        sent = chunk.reshape(group, own, few, wide)
        moved = lax.all_to_all(sent, ("fsdp", "tp"), split_axis=0, concat_axis=0, tiled=True)
        moved = moved.reshape(rows, halves, own, few, wide).transpose(2, 0, 1, 3, 4)
        change = update_matrices(moved).transpose(1, 2, 0, 3, 4).reshape(group, own, few, wide)
        back = lax.all_to_all(change, ("fsdp", "tp"), split_axis=0, concat_axis=0, tiled=True)
        pieces.append(back.reshape(mats // CHUNKS, few, wide))
    new_weights = weight_stack - jnp.concatenate(pieces)
    return (new_weights, new_momentum)


def solution(mesh):
    in_specs = (P("shift", "fsdp", "tp"), P("shift", "fsdp", "tp"), P("shift", "fsdp", "tp"))
    out_specs = (P("shift", "fsdp", "tp"), P("shift", "fsdp", "tp"))
    return jax.shard_map(body, mesh=mesh, in_specs=in_specs, out_specs=out_specs, check_vma=False)
```

```python
import functools

import jax
import jax.numpy as jnp
from jax import lax
from jax.experimental import pallas as pl
from jax.experimental.pallas import tpu as pltpu
from jax.sharding import PartitionSpec as P

ITERS = 3


hold_rate = 0.95
learn_rate = 0.9

ROW_BY_ROW = (((1,), (1,)), ((), ()))
PLAIN = (((1,), (0,)), ((), ()))
dot = functools.partial(lax.dot_general, preferred_element_type=jnp.float32)


def parts_of(value):
    high = value.astype(jnp.bfloat16)
    rest = value - high.astype(jnp.float32)
    middle = rest.astype(jnp.bfloat16)
    low = (rest - middle.astype(jnp.float32)).astype(jnp.bfloat16)
    return high, middle, low


def left_parts(value):
    high, middle, low = parts_of(value)
    return (
        jnp.concatenate([high, high], axis=1),
        jnp.concatenate([middle, middle], axis=1),
        jnp.concatenate([high, low], axis=1),
    )


def right_parts(value):
    high, middle, low = parts_of(value)
    return (
        jnp.concatenate([high, middle], axis=0),
        jnp.concatenate([low, high], axis=0),
    )


def product_of(left, right):
    return (
        dot(left[2], right[1], PLAIN) + dot(left[1], right[0], PLAIN)
    ) + dot(left[0], right[0], PLAIN)


def gram_of(high, middle, low):
    side = high.shape[0]
    first = dot(high, jnp.concatenate([high, middle], axis=0), ROW_BY_ROW)
    small = dot(high, low, ROW_BY_ROW) + first[:, side:]
    return (dot(middle, middle, ROW_BY_ROW) + (small + small.T)) + first[:, :side]


def step_matrices(grams):
    side = grams[0].shape[0]
    row = lax.broadcasted_iota(jnp.int32, (side, side), 0)
    col = lax.broadcasted_iota(jnp.int32, (side, side), 1)
    diagonal = row == col
    inverses = [
        lax.rsqrt(jnp.sum(jnp.where(diagonal, gram, 0.0), axis=(0, 1), keepdims=True) + 1e-06)
        for gram in grams
    ]
    grams = [(gram * inverse) * inverse for gram, inverse in zip(grams, inverses)]
    products = None
    for step in range(ITERS):
        rights = [right_parts(gram) for gram in grams]
        squares = [product_of(left_parts(gram), right) for gram, right in zip(grams, rights)]
        factors = [
            jnp.where(diagonal, 3.4445, 0.0) + (-4.775 * gram + 2.0315 * square)
            for gram, square in zip(grams, squares)
        ]
        lefts = [left_parts(factor) for factor in factors]
        if step < ITERS - 1:
            inner = [product_of(left, right) for left, right in zip(lefts, rights)]
            grams = [product_of(left, right_parts(one)) for left, one in zip(lefts, inner)]
        if products is None:
            products = factors
        else:
            products = [product_of(left, right_parts(one)) for left, one in zip(lefts, products)]
    return [one * (learn_rate * inverse) for one, inverse in zip(products, inverses)]


def matrices_kernel(halves, moved_ref, out_ref, whole_ref):
    senders, own, few, wide = moved_ref.shape
    parts = []
    for mat in range(own):
        for sender in range(senders):
            row, half = divmod(sender, halves)
            whole_ref[mat, row * few : (row + 1) * few, half * wide : (half + 1) * wide] = moved_ref[sender, mat]
        parts.append(parts_of(whole_ref[mat]))
    steps = step_matrices([gram_of(*one) for one in parts])
    for mat, (step, (high, middle, low)) in enumerate(zip(steps, parts)):
        right = (jnp.concatenate([high, middle], axis=0), jnp.concatenate([low, high], axis=0))
        whole_ref[mat] = product_of(left_parts(step), right)
        for sender in range(senders):
            row, half = divmod(sender, halves)
            out_ref[sender, mat] = whole_ref[mat, row * few : (row + 1) * few, half * wide : (half + 1) * wide]


def update_matrices(moved, rows, halves):
    _, own, few, wide = moved.shape
    side, width = rows * few, halves * wide
    flops = own * (6 * 2) * (2 * side * side * width + 9 * side**3)
    return pl.pallas_call(
        functools.partial(matrices_kernel, halves),
        out_shape=jax.ShapeDtypeStruct(moved.shape, jnp.float32),
        in_specs=[pl.BlockSpec(memory_space=pltpu.VMEM)],
        out_specs=pl.BlockSpec(memory_space=pltpu.VMEM),
        scratch_shapes=[pltpu.VMEM((own, side, width), jnp.float32)],
        compiler_params=pltpu.CompilerParams(vmem_limit_bytes=24 << 20),
        cost_estimate=pl.CostEstimate(flops=flops, bytes_accessed=2 * 4 * moved.size, transcendentals=0),
    )(moved)


def body(grad_stack, moment_stack, weight_stack):
    mats, few, wide = grad_stack.shape
    rows, halves = lax.axis_size("fsdp"), lax.axis_size("tp")
    group = rows * halves
    new_momentum = hold_rate * moment_stack + grad_stack
    moved = lax.all_to_all(new_momentum, ("fsdp", "tp"), split_axis=0, concat_axis=0, tiled=True)
    change = update_matrices(moved.reshape(group, mats // group, few, wide), rows, halves)
    back = lax.all_to_all(change.reshape(mats, few, wide), ("fsdp", "tp"), split_axis=0, concat_axis=0, tiled=True)
    new_weights = weight_stack - back
    return (new_weights, new_momentum)


def solution(mesh):
    in_specs = (P("shift", "fsdp", "tp"), P("shift", "fsdp", "tp"), P("shift", "fsdp", "tp"))
    out_specs = (P("shift", "fsdp", "tp"), P("shift", "fsdp", "tp"))
    return jax.shard_map(body, mesh=mesh, in_specs=in_specs, out_specs=out_specs, check_vma=False)
```

```python
import functools

import jax
import jax.numpy as jnp
from jax import lax
from jax.experimental import pallas as pl
from jax.experimental.pallas import tpu as pltpu
from jax.sharding import PartitionSpec as P

ITERS = 3
MOMENTUM_PIECES = 8
WEIGHT_PIECES = 8
GROUP = ("far", "core", "near", "tp")


hold_rate = 0.95
learn_rate = 0.9

ROW_BY_ROW = (((1,), (1,)), ((), ()))
PLAIN = (((1,), (0,)), ((), ()))
dot = functools.partial(lax.dot_general, preferred_element_type=jnp.float32)


def parts_of(value):
    high = value.astype(jnp.bfloat16)
    rest = value - high.astype(jnp.float32)
    middle = rest.astype(jnp.bfloat16)
    low = (rest - middle.astype(jnp.float32)).astype(jnp.bfloat16)
    return high, middle, low


def left_parts(value):
    high, middle, low = parts_of(value)
    return (
        jnp.concatenate([high, high], axis=1),
        jnp.concatenate([middle, middle], axis=1),
        jnp.concatenate([high, low], axis=1),
    )


def right_parts(value):
    high, middle, low = parts_of(value)
    return (
        jnp.concatenate([high, middle], axis=0),
        jnp.concatenate([low, high], axis=0),
    )


def product_of(left, right):
    return (
        dot(left[2], right[1], PLAIN) + dot(left[1], right[0], PLAIN)
    ) + dot(left[0], right[0], PLAIN)


def gram_of(high, middle, low):
    side = high.shape[0]
    first = dot(high, jnp.concatenate([high, middle], axis=0), ROW_BY_ROW)
    small = dot(high, low, ROW_BY_ROW) + first[:, side:]
    return (dot(middle, middle, ROW_BY_ROW) + (small + small.T)) + first[:, :side]


def step_matrices(grams):
    side = grams[0].shape[0]
    row = lax.broadcasted_iota(jnp.int32, (side, side), 0)
    col = lax.broadcasted_iota(jnp.int32, (side, side), 1)
    diagonal = row == col
    inverses = [
        lax.rsqrt(jnp.sum(jnp.where(diagonal, gram, 0.0), axis=(0, 1), keepdims=True) + 1e-06)
        for gram in grams
    ]
    grams = [(gram * inverse) * inverse for gram, inverse in zip(grams, inverses)]
    products = None
    for step in range(ITERS):
        rights = [right_parts(gram) for gram in grams]
        squares = [product_of(left_parts(gram), right) for gram, right in zip(grams, rights)]
        factors = [
            jnp.where(diagonal, 3.4445, 0.0) + (-4.775 * gram + 2.0315 * square)
            for gram, square in zip(grams, squares)
        ]
        lefts = [left_parts(factor) for factor in factors]
        if step < ITERS - 1:
            inner = [product_of(left, right) for left, right in zip(lefts, rights)]
            grams = [product_of(left, right_parts(one)) for left, one in zip(lefts, inner)]
        if products is None:
            products = factors
        else:
            products = [product_of(left, right_parts(one)) for left, one in zip(lefts, products)]
    return [one * (learn_rate * inverse) for one, inverse in zip(products, inverses)]


def matrices_kernel(halves, moved_ref, sent_ref, out_ref, kept_ref, whole_ref, sem):
    senders, own, few, wide = moved_ref.shape
    keep = pltpu.make_async_copy(sent_ref, kept_ref, sem)
    keep.start()
    parts = []
    for mat in range(own):
        for sender in range(senders):
            row, half = divmod(sender, halves)
            whole_ref[mat, row * few : (row + 1) * few, half * wide : (half + 1) * wide] = moved_ref[sender, mat]
        parts.append(parts_of(whole_ref[mat]))
    steps = step_matrices([gram_of(*one) for one in parts])
    for mat, (step, (high, middle, low)) in enumerate(zip(steps, parts)):
        right = (jnp.concatenate([high, middle], axis=0), jnp.concatenate([low, high], axis=0))
        change = product_of(left_parts(step), right)
        for sender in range(senders):
            row, half = divmod(sender, halves)
            out_ref[sender, mat] = change[row * few : (row + 1) * few, half * wide : (half + 1) * wide]
    keep.wait()


def update_matrices(moved, sent, rows, halves):
    _, own, few, wide = moved.shape
    side, width = rows * few, halves * wide
    flops = own * (6 * 2) * (2 * side * side * width + 9 * side**3)
    return pl.pallas_call(
        functools.partial(matrices_kernel, halves),
        out_shape=[jax.ShapeDtypeStruct(moved.shape, jnp.float32), jax.ShapeDtypeStruct(sent.shape, jnp.float32)],
        in_specs=[pl.BlockSpec(memory_space=pltpu.VMEM)] * 2,
        out_specs=[pl.BlockSpec(memory_space=pltpu.VMEM), pl.BlockSpec(memory_space=pl.ANY)],
        scratch_shapes=[pltpu.VMEM((own, side, width), jnp.float32), pltpu.SemaphoreType.DMA],
        compiler_params=pltpu.CompilerParams(vmem_limit_bytes=24 << 20),
        cost_estimate=pl.CostEstimate(flops=flops, bytes_accessed=2 * 4 * moved.size, transcendentals=0),
    )(moved, sent)


def momentum_kernel(grad_ref, moment_ref, out_ref, grads, moments, sems):
    pieces, span = grads.shape[:2]
    copies = []
    for piece in range(pieces):
        mine = pl.ds(piece * span, span)
        pair = (
            pltpu.make_async_copy(moment_ref.at[mine], moments.at[piece], sems.at[piece, 0]),
            pltpu.make_async_copy(grad_ref.at[mine], grads.at[piece], sems.at[piece, 1]),
        )
        for copy in pair:
            copy.start()
        copies.append(pair)
    for piece, pair in enumerate(copies):
        for copy in pair:
            copy.wait()
        out_ref[piece * span : (piece + 1) * span] = hold_rate * moments[piece] + grads[piece]


def momentum_of(grad, moment):
    mats, few, wide = grad.shape
    pieces = (MOMENTUM_PIECES, mats // MOMENTUM_PIECES, few, wide)
    anywhere = pl.BlockSpec(memory_space=pl.ANY)
    return pl.pallas_call(
        momentum_kernel,
        out_shape=jax.ShapeDtypeStruct(grad.shape, jnp.float32),
        in_specs=[anywhere, anywhere],
        out_specs=pl.BlockSpec(memory_space=pltpu.VMEM),
        scratch_shapes=[
            pltpu.VMEM(pieces, jnp.float32),
            pltpu.VMEM(pieces, jnp.float32),
            pltpu.SemaphoreType.DMA((MOMENTUM_PIECES, 2)),
        ],
        compiler_params=pltpu.CompilerParams(vmem_limit_bytes=16 << 20),
        cost_estimate=pl.CostEstimate(flops=2 * grad.size, bytes_accessed=2 * 4 * grad.size, transcendentals=0),
    )(
        pltpu.with_memory_space_constraint(grad, pltpu.HBM),
        pltpu.with_memory_space_constraint(moment, pltpu.HBM),
    )


def weights_kernel(weight_ref, back_ref, out_ref, news, sems):
    pieces, span = news.shape[:2]
    copies = []
    for piece in range(pieces):
        mine = slice(piece * span, (piece + 1) * span)
        news[piece] = weight_ref[mine] - back_ref[mine]
        copy = pltpu.make_async_copy(news.at[piece], out_ref.at[pl.ds(piece * span, span)], sems.at[piece])
        copy.start()
        copies.append(copy)
    for copy in copies:
        copy.wait()


def weights_of(weight, back):
    mats, few, wide = weight.shape
    whole = pl.BlockSpec(memory_space=pltpu.VMEM)
    return pl.pallas_call(
        weights_kernel,
        out_shape=jax.ShapeDtypeStruct(weight.shape, jnp.float32),
        in_specs=[whole, whole],
        out_specs=pl.BlockSpec(memory_space=pl.ANY),
        scratch_shapes=[
            pltpu.VMEM((WEIGHT_PIECES, mats // WEIGHT_PIECES, few, wide), jnp.float32),
            pltpu.SemaphoreType.DMA((WEIGHT_PIECES,)),
        ],
        compiler_params=pltpu.CompilerParams(vmem_limit_bytes=16 << 20),
        cost_estimate=pl.CostEstimate(flops=weight.size, bytes_accessed=4 * weight.size, transcendentals=0),
    )(weight, back)


def body(grad_stack, moment_stack, weight_stack):
    mats, few, wide = grad_stack.shape
    group, halves = lax.axis_size(GROUP), lax.axis_size(GROUP[-1])
    sent = momentum_of(grad_stack, moment_stack)
    moved = lax.all_to_all(sent, GROUP, split_axis=0, concat_axis=0, tiled=True)
    moved = moved.reshape(group, mats // group, few, wide)
    change, new_momentum = update_matrices(moved, sent, group // halves, halves)
    back = lax.all_to_all(change.reshape(mats, few, wide), GROUP, split_axis=0, concat_axis=0, tiled=True)
    return (weights_of(weight_stack, back), new_momentum)


def solution(mesh):
    shift, fsdp, tp = mesh.devices.shape
    fine = jax.sharding.Mesh(mesh.devices.reshape(shift, fsdp // 4, 2, 2, tp), ("shift", "far", "near", "core", "tp"))
    spec = P("shift", ("far", "near", "core"), "tp")
    return jax.shard_map(body, mesh=fine, in_specs=(spec,) * 3, out_specs=(spec,) * 2, check_vma=False)
```

```python
import functools

import jax
import jax.numpy as jnp
from jax import lax
from jax.experimental import pallas as pl
from jax.experimental.pallas import tpu as pltpu
from jax.sharding import PartitionSpec as P

ITERS = 3
MOMENTUM_PIECES = 4
WEIGHT_PIECES = 4
GROUP = ("far", "core", "near", "tp")


hold_rate = 0.95
learn_rate = 0.9

ROW_BY_ROW = (((1,), (1,)), ((), ()))
PLAIN = (((1,), (0,)), ((), ()))
dot = functools.partial(lax.dot_general, preferred_element_type=jnp.float32)


def parts_of(value):
    high = value.astype(jnp.bfloat16)
    rest = value - high.astype(jnp.float32)
    middle = rest.astype(jnp.bfloat16)
    low = (rest - middle.astype(jnp.float32)).astype(jnp.bfloat16)
    return high, middle, low


def left_parts(value):
    high, middle, low = parts_of(value)
    return (
        jnp.concatenate([high, high], axis=1),
        jnp.concatenate([middle, middle], axis=1),
        jnp.concatenate([high, low], axis=1),
    )


def right_parts(value):
    high, middle, low = parts_of(value)
    return (
        jnp.concatenate([high, middle], axis=0),
        jnp.concatenate([low, high], axis=0),
    )


def product_of(left, right):
    return (
        dot(left[2], right[1], PLAIN) + dot(left[1], right[0], PLAIN)
    ) + dot(left[0], right[0], PLAIN)


def gram_of(high, middle, low):
    side = high.shape[0]
    first = dot(high, jnp.concatenate([high, middle], axis=0), ROW_BY_ROW)
    small = dot(high, low, ROW_BY_ROW) + first[:, side:]
    return (dot(middle, middle, ROW_BY_ROW) + (small + small.T)) + first[:, :side]


def step_matrices(grams):
    side = grams[0].shape[0]
    row = lax.broadcasted_iota(jnp.int32, (side, side), 0)
    col = lax.broadcasted_iota(jnp.int32, (side, side), 1)
    diagonal = row == col
    inverses = [
        lax.rsqrt(jnp.sum(jnp.where(diagonal, gram, 0.0), axis=(0, 1), keepdims=True) + 1e-06)
        for gram in grams
    ]
    grams = [(gram * inverse) * inverse for gram, inverse in zip(grams, inverses)]
    products = None
    for step in range(ITERS):
        rights = [right_parts(gram) for gram in grams]
        squares = [product_of(left_parts(gram), right) for gram, right in zip(grams, rights)]
        factors = [
            jnp.where(diagonal, 3.4445, 0.0) + (-4.775 * gram + 2.0315 * square)
            for gram, square in zip(grams, squares)
        ]
        lefts = [left_parts(factor) for factor in factors]
        if step < ITERS - 1:
            inner = [product_of(left, right) for left, right in zip(lefts, rights)]
            grams = [product_of(left, right_parts(one)) for left, one in zip(lefts, inner)]
        if products is None:
            products = factors
        else:
            products = [product_of(left, right_parts(one)) for left, one in zip(lefts, products)]
    return [one * (learn_rate * inverse) for one, inverse in zip(products, inverses)]


def matrices_kernel(halves, moved_ref, sent_ref, out_ref, kept_ref, whole_ref, sem):
    senders, own, few, wide = moved_ref.shape
    keep = pltpu.make_async_copy(sent_ref, kept_ref, sem)
    keep.start()
    parts = []
    for mat in range(own):
        for sender in range(senders):
            row, half = divmod(sender, halves)
            whole_ref[mat, row * few : (row + 1) * few, half * wide : (half + 1) * wide] = moved_ref[sender, mat]
        parts.append(parts_of(whole_ref[mat]))
    steps = step_matrices([gram_of(*one) for one in parts])
    for mat, (step, (high, middle, low)) in enumerate(zip(steps, parts)):
        step_high, step_middle, _ = parts_of(step)
        change = dot(step_high, middle, PLAIN) + dot(
            jnp.concatenate([step_high, step_middle], axis=1), jnp.concatenate([high, high], axis=0), PLAIN
        )
        for sender in range(senders):
            row, half = divmod(sender, halves)
            out_ref[sender, mat] = change[row * few : (row + 1) * few, half * wide : (half + 1) * wide]
    keep.wait()


def update_matrices(moved, sent, rows, halves):
    _, own, few, wide = moved.shape
    side, width = rows * few, halves * wide
    flops = own * (6 * 2) * (2 * side * side * width + 9 * side**3)
    return pl.pallas_call(
        functools.partial(matrices_kernel, halves),
        out_shape=[jax.ShapeDtypeStruct(moved.shape, jnp.float32), jax.ShapeDtypeStruct(sent.shape, jnp.float32)],
        in_specs=[pl.BlockSpec(memory_space=pltpu.VMEM)] * 2,
        out_specs=[pl.BlockSpec(memory_space=pltpu.VMEM), pl.BlockSpec(memory_space=pl.ANY)],
        scratch_shapes=[pltpu.VMEM((own, side, width), jnp.float32), pltpu.SemaphoreType.DMA],
        compiler_params=pltpu.CompilerParams(vmem_limit_bytes=24 << 20),
        cost_estimate=pl.CostEstimate(flops=flops, bytes_accessed=2 * 4 * moved.size, transcendentals=0),
    )(moved, sent)


def momentum_kernel(grad_ref, moment_ref, out_ref, grads, moments, sems):
    pieces, span = grads.shape[:2]
    copies = []
    for piece in range(pieces):
        mine = pl.ds(piece * span, span)
        pair = (
            pltpu.make_async_copy(moment_ref.at[mine], moments.at[piece], sems.at[piece, 0]),
            pltpu.make_async_copy(grad_ref.at[mine], grads.at[piece], sems.at[piece, 1]),
        )
        for copy in pair:
            copy.start()
        copies.append(pair)
    for piece, pair in enumerate(copies):
        for copy in pair:
            copy.wait()
        out_ref[piece * span : (piece + 1) * span] = hold_rate * moments[piece] + grads[piece]


def momentum_of(grad, moment):
    mats, few, wide = grad.shape
    pieces = (MOMENTUM_PIECES, mats // MOMENTUM_PIECES, few, wide)
    anywhere = pl.BlockSpec(memory_space=pl.ANY)
    return pl.pallas_call(
        momentum_kernel,
        out_shape=jax.ShapeDtypeStruct(grad.shape, jnp.float32),
        in_specs=[anywhere, anywhere],
        out_specs=pl.BlockSpec(memory_space=pltpu.VMEM),
        scratch_shapes=[
            pltpu.VMEM(pieces, jnp.float32),
            pltpu.VMEM(pieces, jnp.float32),
            pltpu.SemaphoreType.DMA((MOMENTUM_PIECES, 2)),
        ],
        compiler_params=pltpu.CompilerParams(vmem_limit_bytes=16 << 20),
        cost_estimate=pl.CostEstimate(flops=2 * grad.size, bytes_accessed=2 * 4 * grad.size, transcendentals=0),
    )(
        pltpu.with_memory_space_constraint(grad, pltpu.HBM),
        pltpu.with_memory_space_constraint(moment, pltpu.HBM),
    )


def weights_kernel(weight_ref, back_ref, out_ref, news, sems):
    pieces, span = news.shape[:2]
    copies = []
    for piece in range(pieces):
        mine = slice(piece * span, (piece + 1) * span)
        news[piece] = weight_ref[mine] - back_ref[mine]
        copy = pltpu.make_async_copy(news.at[piece], out_ref.at[pl.ds(piece * span, span)], sems.at[piece])
        copy.start()
        copies.append(copy)
    for copy in copies:
        copy.wait()


def weights_of(weight, back):
    mats, few, wide = weight.shape
    whole = pl.BlockSpec(memory_space=pltpu.VMEM)
    return pl.pallas_call(
        weights_kernel,
        out_shape=jax.ShapeDtypeStruct(weight.shape, jnp.float32),
        in_specs=[whole, whole],
        out_specs=pl.BlockSpec(memory_space=pl.ANY),
        scratch_shapes=[
            pltpu.VMEM((WEIGHT_PIECES, mats // WEIGHT_PIECES, few, wide), jnp.float32),
            pltpu.SemaphoreType.DMA((WEIGHT_PIECES,)),
        ],
        compiler_params=pltpu.CompilerParams(vmem_limit_bytes=16 << 20),
        cost_estimate=pl.CostEstimate(flops=weight.size, bytes_accessed=4 * weight.size, transcendentals=0),
    )(weight, back)


def body(grad_stack, moment_stack, weight_stack):
    mats, few, wide = grad_stack.shape
    group, halves = lax.axis_size(GROUP), lax.axis_size(GROUP[-1])
    sent = momentum_of(grad_stack, moment_stack)
    moved = lax.all_to_all(sent, GROUP, split_axis=0, concat_axis=0, tiled=True)
    moved = moved.reshape(group, mats // group, few, wide)
    change, new_momentum = update_matrices(moved, sent, group // halves, halves)
    back = lax.all_to_all(change.reshape(mats, few, wide), GROUP, split_axis=0, concat_axis=0, tiled=True)
    return (weights_of(weight_stack, back), new_momentum)


def solution(mesh):
    shift, fsdp, tp = mesh.devices.shape
    fine = jax.sharding.Mesh(mesh.devices.reshape(shift, fsdp // 4, 2, 2, tp), ("shift", "far", "near", "core", "tp"))
    spec = P("shift", ("far", "near", "core"), "tp")
    return jax.shard_map(body, mesh=fine, in_specs=(spec,) * 3, out_specs=(spec,) * 2, check_vma=False)
```

```python
import functools

import jax
import jax.numpy as jnp
from jax import lax
from jax.experimental import pallas as pl
from jax.experimental.pallas import tpu as pltpu
from jax.sharding import PartitionSpec as P

ITERS = 3
MOMENTUM_PIECES = 8
WEIGHT_PIECES = 8
GROUP = ("far", "core", "near", "tp")


hold_rate = 0.95
learn_rate = 0.9

ROW_BY_ROW = (((1,), (1,)), ((), ()))
PLAIN = (((1,), (0,)), ((), ()))
dot = functools.partial(lax.dot_general, preferred_element_type=jnp.float32)


def parts_of(value):
    high = value.astype(jnp.bfloat16)
    rest = value - high.astype(jnp.float32)
    middle = rest.astype(jnp.bfloat16)
    low = (rest - middle.astype(jnp.float32)).astype(jnp.bfloat16)
    return high, middle, low


def left_parts(value):
    high, middle, low = parts_of(value)
    return (
        jnp.concatenate([high, high], axis=1),
        jnp.concatenate([middle, middle], axis=1),
        jnp.concatenate([high, low], axis=1),
    )


def right_parts(value):
    high, middle, low = parts_of(value)
    return (
        jnp.concatenate([high, middle], axis=0),
        jnp.concatenate([low, high], axis=0),
    )


def product_of(left, right):
    return (
        dot(left[2], right[1], PLAIN) + dot(left[1], right[0], PLAIN)
    ) + dot(left[0], right[0], PLAIN)


def gram_of(high, middle, low):
    side = high.shape[0]
    first = dot(high, jnp.concatenate([high, middle], axis=0), ROW_BY_ROW)
    small = dot(high, low, ROW_BY_ROW) + first[:, side:]
    return (dot(middle, middle, ROW_BY_ROW) + (small + small.T)) + first[:, :side]


def step_matrices(grams):
    side = grams[0].shape[0]
    row = lax.broadcasted_iota(jnp.int32, (side, side), 0)
    col = lax.broadcasted_iota(jnp.int32, (side, side), 1)
    diagonal = row == col
    inverses = [
        lax.rsqrt(jnp.sum(jnp.where(diagonal, gram, 0.0), axis=(0, 1), keepdims=True) + 1e-06)
        for gram in grams
    ]
    grams = [(gram * inverse) * inverse for gram, inverse in zip(grams, inverses)]
    products = None
    for step in range(ITERS):
        rights = [right_parts(gram) for gram in grams]
        squares = [product_of(left_parts(gram), right) for gram, right in zip(grams, rights)]
        factors = [
            jnp.where(diagonal, 3.4445, 0.0) + (-4.775 * gram + 2.0315 * square)
            for gram, square in zip(grams, squares)
        ]
        lefts = [left_parts(factor) for factor in factors]
        if step < ITERS - 1:
            inner = [product_of(left, right) for left, right in zip(lefts, rights)]
            grams = [product_of(left, right_parts(one)) for left, one in zip(lefts, inner)]
        if products is None:
            products = factors
        else:
            products = [product_of(left, right_parts(one)) for left, one in zip(lefts, products)]
    return [one * (learn_rate * inverse) for one, inverse in zip(products, inverses)]


def matrices_kernel(halves, moved_ref, sent_ref, out_ref, kept_ref, whole_ref, sem):
    senders, own, few, wide = moved_ref.shape
    keep = pltpu.make_async_copy(sent_ref, kept_ref, sem)
    keep.start()
    parts = []
    for mat in range(own):
        for sender in range(senders):
            row, half = divmod(sender, halves)
            whole_ref[mat, row * few : (row + 1) * few, half * wide : (half + 1) * wide] = moved_ref[sender, mat]
        parts.append(parts_of(whole_ref[mat]))
    steps = step_matrices([gram_of(*one) for one in parts])
    for mat, (step, (high, middle, low)) in enumerate(zip(steps, parts)):
        right = (jnp.concatenate([high, middle], axis=0), jnp.concatenate([low, high], axis=0))
        change = product_of(left_parts(step), right)
        for sender in range(senders):
            row, half = divmod(sender, halves)
            out_ref[sender, mat] = change[row * few : (row + 1) * few, half * wide : (half + 1) * wide]
    keep.wait()


def update_matrices(moved, sent, rows, halves):
    _, own, few, wide = moved.shape
    side, width = rows * few, halves * wide
    flops = own * (6 * 2) * (2 * side * side * width + 9 * side**3)
    return pl.pallas_call(
        functools.partial(matrices_kernel, halves),
        out_shape=[jax.ShapeDtypeStruct(moved.shape, jnp.float32), jax.ShapeDtypeStruct(sent.shape, jnp.float32)],
        in_specs=[pl.BlockSpec(memory_space=pltpu.VMEM)] * 2,
        out_specs=[pl.BlockSpec(memory_space=pltpu.VMEM), pl.BlockSpec(memory_space=pl.ANY)],
        scratch_shapes=[pltpu.VMEM((own, side, width), jnp.float32), pltpu.SemaphoreType.DMA],
        compiler_params=pltpu.CompilerParams(vmem_limit_bytes=24 << 20),
        cost_estimate=pl.CostEstimate(flops=flops, bytes_accessed=2 * 4 * moved.size, transcendentals=0),
    )(moved, sent)


def momentum_kernel(grad_ref, moment_ref, out_ref, grads, moments, sems):
    pieces, span = grads.shape[:2]
    copies = []
    for piece in range(pieces):
        mine = pl.ds(piece * span, span)
        pair = (
            pltpu.make_async_copy(moment_ref.at[mine], moments.at[piece], sems.at[piece, 0]),
            pltpu.make_async_copy(grad_ref.at[mine], grads.at[piece], sems.at[piece, 1]),
        )
        for copy in pair:
            copy.start()
        copies.append(pair)
    for piece, pair in enumerate(copies):
        for copy in pair:
            copy.wait()
        out_ref[piece * span : (piece + 1) * span] = hold_rate * moments[piece] + grads[piece]


def momentum_of(grad, moment):
    mats, few, wide = grad.shape
    pieces = (MOMENTUM_PIECES, mats // MOMENTUM_PIECES, few, wide)
    anywhere = pl.BlockSpec(memory_space=pl.ANY)
    return pl.pallas_call(
        momentum_kernel,
        out_shape=jax.ShapeDtypeStruct(grad.shape, jnp.float32),
        in_specs=[anywhere, anywhere],
        out_specs=pl.BlockSpec(memory_space=pltpu.VMEM),
        scratch_shapes=[
            pltpu.VMEM(pieces, jnp.float32),
            pltpu.VMEM(pieces, jnp.float32),
            pltpu.SemaphoreType.DMA((MOMENTUM_PIECES, 2)),
        ],
        compiler_params=pltpu.CompilerParams(vmem_limit_bytes=16 << 20),
        cost_estimate=pl.CostEstimate(flops=2 * grad.size, bytes_accessed=2 * 4 * grad.size, transcendentals=0),
    )(
        pltpu.with_memory_space_constraint(grad, pltpu.HBM),
        pltpu.with_memory_space_constraint(moment, pltpu.HBM),
    )


def weights_kernel(weight_ref, back_ref, out_ref, news, sems):
    pieces, span = news.shape[:2]
    copies = []
    for piece in range(pieces):
        mine = slice(piece * span, (piece + 1) * span)
        news[piece] = weight_ref[mine] - back_ref[mine]
        copy = pltpu.make_async_copy(news.at[piece], out_ref.at[pl.ds(piece * span, span)], sems.at[piece])
        copy.start()
        copies.append(copy)
    for copy in copies:
        copy.wait()


def weights_of(weight, back):
    mats, few, wide = weight.shape
    whole = pl.BlockSpec(memory_space=pltpu.VMEM)
    return pl.pallas_call(
        weights_kernel,
        out_shape=jax.ShapeDtypeStruct(weight.shape, jnp.float32),
        in_specs=[whole, whole],
        out_specs=pl.BlockSpec(memory_space=pl.ANY),
        scratch_shapes=[
            pltpu.VMEM((WEIGHT_PIECES, mats // WEIGHT_PIECES, few, wide), jnp.float32),
            pltpu.SemaphoreType.DMA((WEIGHT_PIECES,)),
        ],
        compiler_params=pltpu.CompilerParams(vmem_limit_bytes=16 << 20),
        cost_estimate=pl.CostEstimate(flops=weight.size, bytes_accessed=4 * weight.size, transcendentals=0),
    )(weight, back)


def body(grad_stack, moment_stack, weight_stack):
    mats, few, wide = grad_stack.shape
    group, halves = lax.axis_size(GROUP), lax.axis_size(GROUP[-1])
    far = lax.axis_size(GROUP[0])
    plane = group // far
    members = [[((z + far // 2) % far) * plane + one for z in range(far) for one in range(plane)]]
    sent = momentum_of(grad_stack, moment_stack)
    moved = lax.all_to_all(sent, GROUP, split_axis=0, concat_axis=0, tiled=True, axis_index_groups=members)
    moved = moved.reshape(group, mats // group, few, wide)
    change, new_momentum = update_matrices(moved, sent, group // halves, halves)
    back = lax.all_to_all(change.reshape(mats, few, wide), GROUP, split_axis=0, concat_axis=0, tiled=True, axis_index_groups=members)
    return (weights_of(weight_stack, back), new_momentum)


def solution(mesh):
    shift, fsdp, tp = mesh.devices.shape
    fine = jax.sharding.Mesh(mesh.devices.reshape(shift, fsdp // 4, 2, 2, tp), ("shift", "far", "near", "core", "tp"))
    spec = P("shift", ("far", "near", "core"), "tp")
    return jax.shard_map(body, mesh=fine, in_specs=(spec,) * 3, out_specs=(spec,) * 2, check_vma=False)
```

```python
import functools

import jax
import jax.numpy as jnp
from jax import lax
from jax.experimental import pallas as pl
from jax.experimental.pallas import tpu as pltpu
from jax.sharding import PartitionSpec as P

ITERS = 3
MOMENTUM_PIECES = 8
WEIGHT_PIECES = 8
GROUP = ("far", "core", "near", "tp")


hold_rate = 0.95
learn_rate = 0.9

ROW_BY_ROW = (((1,), (1,)), ((), ()))
PLAIN = (((1,), (0,)), ((), ()))
dot = functools.partial(lax.dot_general, preferred_element_type=jnp.float32)


def parts_of(value):
    high = value.astype(jnp.bfloat16)
    rest = value - high.astype(jnp.float32)
    middle = rest.astype(jnp.bfloat16)
    low = (rest - middle.astype(jnp.float32)).astype(jnp.bfloat16)
    return high, middle, low


def left_parts(value):
    high, middle, low = parts_of(value)
    return (
        jnp.concatenate([high, high], axis=1),
        jnp.concatenate([middle, middle], axis=1),
        jnp.concatenate([high, low], axis=1),
    )


def right_parts(value):
    high, middle, low = parts_of(value)
    return (
        jnp.concatenate([high, middle], axis=0),
        jnp.concatenate([low, high], axis=0),
    )


def product_of(left, right):
    return (
        dot(left[2], right[1], PLAIN) + dot(left[1], right[0], PLAIN)
    ) + dot(left[0], right[0], PLAIN)


def gram_of(high, middle, low):
    side = high.shape[0]
    first = dot(high, jnp.concatenate([high, middle], axis=0), ROW_BY_ROW)
    small = dot(high, low, ROW_BY_ROW) + first[:, side:]
    return (dot(middle, middle, ROW_BY_ROW) + (small + small.T)) + first[:, :side]


def step_matrices(grams):
    side = grams[0].shape[0]
    row = lax.broadcasted_iota(jnp.int32, (side, side), 0)
    col = lax.broadcasted_iota(jnp.int32, (side, side), 1)
    diagonal = row == col
    inverses = [
        lax.rsqrt(jnp.sum(jnp.where(diagonal, gram, 0.0), axis=(0, 1), keepdims=True) + 1e-06)
        for gram in grams
    ]
    grams = [(gram * inverse) * inverse for gram, inverse in zip(grams, inverses)]
    products = None
    for step in range(ITERS):
        rights = [right_parts(gram) for gram in grams]
        squares = [product_of(left_parts(gram), right) for gram, right in zip(grams, rights)]
        factors = [
            jnp.where(diagonal, 3.4445, 0.0) + (-4.775 * gram + 2.0315 * square)
            for gram, square in zip(grams, squares)
        ]
        lefts = [left_parts(factor) for factor in factors]
        if step < ITERS - 1:
            inner = [product_of(left, right) for left, right in zip(lefts, rights)]
            grams = [product_of(left, right_parts(one)) for left, one in zip(lefts, inner)]
        if products is None:
            products = factors
        else:
            products = [product_of(left, right_parts(one)) for left, one in zip(lefts, products)]
    return [one * (learn_rate * inverse) for one, inverse in zip(products, inverses)]


def matrices_kernel(halves, moved_ref, sent_ref, out_ref, kept_ref, whole_ref, sem):
    senders, own, few, wide = moved_ref.shape
    keep = pltpu.make_async_copy(sent_ref, kept_ref, sem)
    keep.start()
    parts = []
    for mat in range(own):
        for sender in range(senders):
            row, half = divmod(sender, halves)
            whole_ref[mat, row * few : (row + 1) * few, half * wide : (half + 1) * wide] = moved_ref[sender, mat]
        parts.append(parts_of(whole_ref[mat]))
    steps = step_matrices([gram_of(*one) for one in parts])
    for mat, (step, (high, middle, low)) in enumerate(zip(steps, parts)):
        right = (jnp.concatenate([high, middle], axis=0), jnp.concatenate([low, high], axis=0))
        change = product_of(left_parts(step), right)
        for sender in range(senders):
            row, half = divmod(sender, halves)
            out_ref[sender, mat] = change[row * few : (row + 1) * few, half * wide : (half + 1) * wide]
    keep.wait()


def update_matrices(moved, sent, rows, halves):
    _, own, few, wide = moved.shape
    side, width = rows * few, halves * wide
    flops = own * (6 * 2) * (2 * side * side * width + 9 * side**3)
    return pl.pallas_call(
        functools.partial(matrices_kernel, halves),
        out_shape=[jax.ShapeDtypeStruct(moved.shape, jnp.float32), jax.ShapeDtypeStruct(sent.shape, jnp.float32)],
        in_specs=[pl.BlockSpec(memory_space=pltpu.VMEM)] * 2,
        out_specs=[pl.BlockSpec(memory_space=pltpu.VMEM), pl.BlockSpec(memory_space=pl.ANY)],
        scratch_shapes=[pltpu.VMEM((own, side, width), jnp.float32), pltpu.SemaphoreType.DMA],
        compiler_params=pltpu.CompilerParams(vmem_limit_bytes=24 << 20),
        cost_estimate=pl.CostEstimate(flops=flops, bytes_accessed=2 * 4 * moved.size, transcendentals=0),
    )(moved, sent)


def momentum_kernel(grad_ref, moment_ref, out_ref, grads, moments, sems):
    pieces, span = grads.shape[:2]
    copies = []
    for piece in range(pieces):
        mine = pl.ds(piece * span, span)
        pair = (
            pltpu.make_async_copy(moment_ref.at[mine], moments.at[piece], sems.at[piece, 0]),
            pltpu.make_async_copy(grad_ref.at[mine], grads.at[piece], sems.at[piece, 1]),
        )
        for copy in pair:
            copy.start()
        copies.append(pair)
    for piece, pair in enumerate(copies):
        for copy in pair:
            copy.wait()
        out_ref[piece * span : (piece + 1) * span] = hold_rate * moments[piece] + grads[piece]


def momentum_of(grad, moment):
    mats, few, wide = grad.shape
    pieces = (MOMENTUM_PIECES, mats // MOMENTUM_PIECES, few, wide)
    anywhere = pl.BlockSpec(memory_space=pl.ANY)
    return pl.pallas_call(
        momentum_kernel,
        out_shape=jax.ShapeDtypeStruct(grad.shape, jnp.float32),
        in_specs=[anywhere, anywhere],
        out_specs=pl.BlockSpec(memory_space=pltpu.VMEM),
        scratch_shapes=[
            pltpu.VMEM(pieces, jnp.float32),
            pltpu.VMEM(pieces, jnp.float32),
            pltpu.SemaphoreType.DMA((MOMENTUM_PIECES, 2)),
        ],
        compiler_params=pltpu.CompilerParams(vmem_limit_bytes=16 << 20),
        cost_estimate=pl.CostEstimate(flops=2 * grad.size, bytes_accessed=2 * 4 * grad.size, transcendentals=0),
    )(
        pltpu.with_memory_space_constraint(grad, pltpu.HBM),
        pltpu.with_memory_space_constraint(moment, pltpu.HBM),
    )


def weights_kernel(weight_ref, back_ref, out_ref, news, sems):
    pieces, span = news.shape[:2]
    copies = []
    for piece in range(pieces):
        mine = slice(piece * span, (piece + 1) * span)
        news[piece] = weight_ref[mine] - back_ref[mine]
        copy = pltpu.make_async_copy(news.at[piece], out_ref.at[pl.ds(piece * span, span)], sems.at[piece])
        copy.start()
        copies.append(copy)
    for copy in copies:
        copy.wait()


def weights_of(weight, back):
    mats, few, wide = weight.shape
    whole = pl.BlockSpec(memory_space=pltpu.VMEM)
    return pl.pallas_call(
        weights_kernel,
        out_shape=jax.ShapeDtypeStruct(weight.shape, jnp.float32),
        in_specs=[whole, whole],
        out_specs=pl.BlockSpec(memory_space=pl.ANY),
        scratch_shapes=[
            pltpu.VMEM((WEIGHT_PIECES, mats // WEIGHT_PIECES, few, wide), jnp.float32),
            pltpu.SemaphoreType.DMA((WEIGHT_PIECES,)),
        ],
        compiler_params=pltpu.CompilerParams(vmem_limit_bytes=16 << 20),
        cost_estimate=pl.CostEstimate(flops=weight.size, bytes_accessed=4 * weight.size, transcendentals=0),
    )(weight, back)


def body(grad_stack, moment_stack, weight_stack):
    mats, few, wide = grad_stack.shape
    group, halves = lax.axis_size(GROUP), lax.axis_size(GROUP[-1])
    far = lax.axis_size(GROUP[0])
    plane = group // far
    members = [[((z + far // 2 - 1) % far) * plane + one for z in range(far) for one in range(plane)]]
    sent = momentum_of(grad_stack, moment_stack)
    moved = lax.all_to_all(sent, GROUP, split_axis=0, concat_axis=0, tiled=True, axis_index_groups=members)
    moved = moved.reshape(group, mats // group, few, wide)
    change, new_momentum = update_matrices(moved, sent, group // halves, halves)
    back = lax.all_to_all(change.reshape(mats, few, wide), GROUP, split_axis=0, concat_axis=0, tiled=True, axis_index_groups=members)
    return (weights_of(weight_stack, back), new_momentum)


def solution(mesh):
    shift, fsdp, tp = mesh.devices.shape
    fine = jax.sharding.Mesh(mesh.devices.reshape(shift, fsdp // 4, 2, 2, tp), ("shift", "far", "near", "core", "tp"))
    spec = P("shift", ("far", "near", "core"), "tp")
    return jax.shard_map(body, mesh=fine, in_specs=(spec,) * 3, out_specs=(spec,) * 2, check_vma=False)
```
